32 devices in a mesh: shard: 8 (over z, core), context: 2 (over y), tensor: 2 (over x).
Axes of the slice: x: 2, y: 2, z: 4, core: 2. Of those that a mesh axis runs over, the one named last changes fastest.
Arguments:
- states: bfloat16 [8, 1024, 1024], P('shard', 'context'), may hold values from -6 to 6
- encoded: bfloat16 [8, 256, 1024], P('shard', 'context'), may hold values from -6 to 6
- cotangent: bfloat16 [8, 1024, 1024], P('shard', 'context'), may hold values from -6 to 6
- bucket_ids: int32 [1024], replicated, may hold values from 0 to 31, never falling along the last dimension, each value on 1 to 64 neighbouring positions
- norm_gains: bfloat16 [3, 1024], P(None, 'shard'), may hold values from 0.099609375 to 1.8984375
- bias_table: bfloat16 [32, 16], P('shard', 'tensor'), may hold values from -4 to 4
- self_weights: bfloat16 [3, 1024, 1024], P(None, 'shard', 'tensor'), may hold values from -0.09375 to 0.09375
- mixer_weight: bfloat16 [1024, 1024], P('tensor', 'shard'), may hold values from -2 to 2
- cross_weights: bfloat16 [3, 1024, 1024], P(None, 'shard', 'tensor'), may hold values from -0.09375 to 0.09375
- blend_weight: bfloat16 [1024, 1024], P('tensor', 'shard'), may hold values from -2 to 2
- gate_up: bfloat16 [2, 1024, 2816], P(None, 'shard', 'tensor'), may hold values from -0.1875 to 0.1875
- down_weight: bfloat16 [2816, 1024], P('tensor', 'shard'), may hold values from -0.109375 to 0.109375
Outputs:
- output: bfloat16 [8, 1024, 1024], P('shard', 'context')
- states_grad: float32 [8, 1024, 1024], P('shard', 'context')
- encoded_grad: float32 [8, 256, 1024], P('shard', 'context')
- gains_grad: float32 [2, 1024], P(None, 'shard')
- third_gain: float32 [1024], P('shard')
- table_grad: float32 [32, 16], P('shard', 'tensor')
- self_grad: float32 [3, 1024, 1024], P(None, 'shard', 'tensor')
- mixer_grad: float32 [1024, 1024], P('tensor', 'shard')
- cross_grad: float32 [3, 1024, 1024], P(None, 'shard', 'tensor')
- blend_grad: float32 [1024, 1024], P('tensor', 'shard')
- gate_grad: float32 [2, 1024, 2816], P(None, 'shard', 'tensor')
- down_grad: float32 [2816, 1024], P('tensor', 'shard')
The draws below stay inside these ranges and needn't reach their ends.
Inputs may be any that keep to these rules, and one draw needn't show every extreme that they name: bucket_ids never fall as the offset grows; each of the 32 buckets holds 1 to 64 consecutive offsets.
All inputs are finite; a program needn't handle non-finite values.
Results may differ from the reference program's by a relative error of at most 0.04.
Values may be sent and summed in bfloat16 or wider, within the bound.
A program may use at most 192 MiB of HBM per device.

```python
import math
import jax
import jax.numpy as jnp
import numpy as np
from jax import lax

D = 1024
H = 16
DK = 64
FF = 2816
NBUCKET = 32
HD = 1024
SEQ = 1024
ENC = 256
SEQS = 8


def block_scale(key, shape, split, least, top_value):
    def one(dim, blocks):
        draws = jax.random.uniform(jax.random.fold_in(jax.random.fold_in(key, 6), dim), (blocks,), jnp.float32, least / len(split), top_value / len(split))
        return jnp.repeat(jnp.exp(draws), shape[dim] // blocks).reshape((-1,) + (1,) * (len(shape) - dim - 1))

    level = one(*split[0])
    for cut in split[1:]:
        level = level * one(*cut)
    return level


def profile(count, total, most, skew):
    loads = [(1 << 20) // math.isqrt(grade ** skew) + 1 for grade in range(2, count + 1)]
    spare, holding = total - most - (count - 1), [1] * (count - 1)
    while spare > 0:
        candidates = [i for i in range(count - 1) if holding[i] < most]
        whole, budget = sum([loads[i] for i in candidates]), spare
        for i in candidates:
            addition = min(most - holding[i], max(1, budget * loads[i] // whole), spare)
            holding[i] = holding[i] + addition
            spare = spare - addition
    return np.array([most] + holding)


def ragged(stream_key, amount, total, reach, skew):
    if amount == 2:
        one = jax.random.randint(stream_key, (), max(1, total - reach), min(reach, total - 1) + 1)
        return jnp.stack([one, total - one])
    sizes = jnp.asarray(profile(amount, total, reach, skew), jnp.int32)
    pairs = (amount - 1) // 2
    giver, sink = sizes[1:1 + 2 * pairs:2], sizes[2:2 + 2 * pairs:2]
    slack = jnp.minimum(giver - 1, reach - sink)
    shifted = jax.random.randint(jax.random.fold_in(stream_key, 1), (pairs,), 0, 1 << 20) % (slack + 1)
    sizes = sizes.at[1:1 + 2 * pairs:2].set(giver - shifted).at[2:2 + 2 * pairs:2].set(sink + shifted)
    return sizes[jax.random.permutation(jax.random.fold_in(stream_key, 2), amount)]


def scatter_about(key, extent, spread, bound, split=(), kind=jnp.bfloat16):
    loudness = block_scale(key, extent, split, -0.22, 0.18) if split else 1.0
    entries = jax.random.normal(key, extent, jnp.float32) * spread * loudness
    return jnp.minimum(jnp.maximum(entries, -bound), bound).astype(kind)


def setup_inputs(seed: int = 0) -> dict:
    streams_of = jax.random.split(jax.random.key(seed), 13)
    return {
        "states": scatter_about(streams_of[0], (SEQS, SEQ, D), 1.0, 6.0, ((0, 8), (1, 2))),
        "encoded": scatter_about(streams_of[1], (SEQS, ENC, D), 1.0, 6.0, ((0, 8), (1, 2))),
        "cotangent": scatter_about(streams_of[2], (SEQS, SEQ, D), 1.0, 6.0, ((0, 8), (1, 2))),
        "bucket_ids": jnp.searchsorted(jnp.cumsum(ragged(streams_of[3], NBUCKET, SEQ, 2 * SEQ // NBUCKET, 2)), jnp.arange(SEQ), side="right").astype(jnp.int32),
        "norm_gains": jnp.clip(1.0 + 0.18 * jax.random.normal(streams_of[4], (3, D), jnp.float32), 0.099609375, 1.8984375).astype(jnp.bfloat16),
        "bias_table": scatter_about(streams_of[5], (NBUCKET, H), 1.0, 4.0, ((0, 8), (1, 2))),
        "self_weights": scatter_about(streams_of[6], (3, D, HD), (4 * D) ** -0.5, 0.09375, ((1, 8), (2, 2))),
        "mixer_weight": scatter_about(streams_of[7], (HD, D), (max(8, HD // 128)) ** -0.5, 2.0, ((0, 2), (1, 8))),
        "cross_weights": scatter_about(streams_of[8], (3, D, HD), (4 * D) ** -0.5, 0.09375, ((1, 8), (2, 2))),
        "blend_weight": scatter_about(streams_of[9], (HD, D), (max(8, HD // 128)) ** -0.5, 2.0, ((0, 2), (1, 8))),
        "gate_up": scatter_about(streams_of[10], (2, D, FF), D ** -0.5, 0.1875, ((1, 8), (2, 2))),
        "down_weight": scatter_about(streams_of[11], (FF, D), FF ** -0.5, 0.109375, ((0, 2), (1, 8))),
    }


EPSILON = 1e-06
NEGATIVE = -1e+30
ROOT_TWO_PI = math.sqrt(2.0 / math.pi)

@jax.custom_vjp
def low(v):
    return lax.optimization_barrier(v.astype(jnp.bfloat16)).astype(jnp.float32)

@jax.custom_vjp
def low_back(v):
    return v

def low_keep(v):
    return (low(v), None)

def low_pass(kept, grad):
    return (grad,)

def back_keep(v):
    return (v, None)

def back_low(kept, grad):
    return (low(grad),)
low.defvjp(low_keep, low_pass)
low_back.defvjp(back_keep, back_low)

def normalize(values, gain):
    return values * lax.rsqrt(lax.optimization_barrier(jnp.mean(values * values, axis=-1, keepdims=True)) + EPSILON) * gain

def geglu(gate, upper):
    inner = ROOT_TWO_PI * (gate + 0.044715 * gate * gate * gate)
    return 0.5 * gate * (1.0 + jnp.tanh(inner)) * upper

def product(left, right):
    return jnp.dot(left, right, precision=lax.Precision.HIGHEST)

def attention(query, keys, values, lines):
    total_rows = query.shape[0]
    width = keys.shape[0]
    rows = min(512, total_rows)
    count = total_rows // rows

    def block(index):
        start = index * rows
        part = lax.dynamic_slice_in_dim(query, start, rows, 0)
        scores = jnp.einsum('qhd,khd->hqk', part, keys, precision=lax.Precision.HIGHEST)
        if lines is not None:
            places = start + jnp.arange(rows, dtype=jnp.int32)
            offsets = places[:, None] - jnp.arange(width, dtype=jnp.int32)[None, :]
            bias = jnp.take(lines, jnp.clip(offsets, 0, width - 1), axis=0)
            scores = low_back(scores + jnp.transpose(bias, (2, 0, 1)))
            scores = jnp.where((offsets >= 0)[None, :, :], scores, NEGATIVE)
        else:
            scores = low_back(scores)
        peak = lax.optimization_barrier(jnp.max(scores, axis=-1, keepdims=True))
        raised = jnp.exp(scores - peak)
        probs = low(raised / lax.optimization_barrier(jnp.sum(raised, axis=-1, keepdims=True)))
        return jnp.einsum('hqk,khd->qhd', probs, values, precision=lax.Precision.HIGHEST)
    results = lax.map(jax.checkpoint(block), jnp.arange(count, dtype=jnp.int32))
    return results.reshape(total_rows, -1)

def sequence(weights, rows_in, sources, bucket_ids):
    gains, table, selfs, mixer, crosses, blend, gates, down = weights
    length = rows_in.shape[0]
    source_length = sources.shape[0]
    first_norm = low(normalize(rows_in, gains[0]))
    query = low_back(low(product(first_norm, selfs[0]))).reshape(length, H, DK)
    keys = low_back(low(product(first_norm, selfs[1]))).reshape(length, H, DK)
    values = low_back(low(product(first_norm, selfs[2]))).reshape(length, H, DK)
    lines = jnp.take(table, bucket_ids, axis=0)
    attended = low_back(low(attention(query, keys, values, lines)))
    after = rows_in + low_back(product(attended, mixer))
    second_norm = low(normalize(after, gains[1]))
    cross_query = low_back(low(product(second_norm, crosses[0]))).reshape(length, H, DK)
    source_keys = low_back(low(product(sources, crosses[1]))).reshape(source_length, H, DK)
    source_values = low_back(low(product(sources, crosses[2]))).reshape(source_length, H, DK)
    cross_attended = low_back(low(attention(cross_query, source_keys, source_values, None)))
    middle = after + low_back(product(cross_attended, blend))
    third_norm = low(normalize(middle, gains[2]))
    gate = low_back(product(third_norm, gates[0]))
    upper = low_back(product(third_norm, gates[1]))
    hidden = low(geglu(gate, upper))
    return middle + low_back(product(hidden, down))

def reference(states, encoded, cotangent, bucket_ids, norm_gains, bias_table, self_weights, mixer_weight, cross_weights, blend_weight, gate_up, down_weight):
    params = (norm_gains.astype(jnp.float32), bias_table.astype(jnp.float32), self_weights.astype(jnp.float32), mixer_weight.astype(jnp.float32), cross_weights.astype(jnp.float32), blend_weight.astype(jnp.float32), gate_up.astype(jnp.float32), down_weight.astype(jnp.float32))
    rows_all = states.astype(jnp.float32)
    sources_all = encoded.astype(jnp.float32)
    stepper = jax.checkpoint(sequence)

    def whole(weights, inputs, sources):
        return lax.map(lambda pair: stepper(weights, pair[0], pair[1], bucket_ids), (inputs, sources))
    result, pullback = jax.vjp(whole, params, rows_all, sources_all)
    weight_grads, states_grad, encoded_grad = pullback(cotangent.astype(jnp.float32))
    return (result.astype(jnp.bfloat16), states_grad, encoded_grad, weight_grads[0][:2], weight_grads[0][2], weight_grads[1], weight_grads[2], weight_grads[3], weight_grads[4], weight_grads[5], weight_grads[6], weight_grads[7])
```

```python
import functools
import math

import jax
import jax.numpy as jnp
from jax import lax
from jax.experimental import pallas as pl
from jax.experimental.pallas import tpu as pltpu
from jax.sharding import PartitionSpec as P

DK = 64
PAIR = 2 * DK
TILE = 128


EPSILON = 1e-06
NEGATIVE = -1e30
ROOT_TWO_PI = math.sqrt(2.0 / math.pi)
LOW = jnp.bfloat16
WIDE = jnp.float32


def normalize(values, gain):
    return values * lax.rsqrt(jnp.mean(values * values, axis=-1, keepdims=True) + EPSILON) * gain


def geglu(gate, upper):
    inner = ROOT_TWO_PI * (gate + 0.044715 * gate * gate * gate)
    return 0.5 * gate * (1.0 + jnp.tanh(inner)) * upper


def matmul(left, right):
    return jnp.dot(left, right, preferred_element_type=WIDE)


def left_contract(left, right):
    return lax.dot_general(left, right, (((0,), (0,)), ((), ())), preferred_element_type=WIDE)


def right_contract(left, right):
    return lax.dot_general(left, right, (((1,), (1,)), ((), ())), preferred_element_type=WIDE)


def shifted(value, axis, step):
    count = lax.axis_size(axis)
    return lax.ppermute(value, axis, [(i, (i + step) % count) for i in range(count)])


def pair_sum(part, axis):
    low = part.astype(LOW)
    if lax.axis_size(axis) == 2:
        return low.astype(WIDE) + shifted(low, axis, 1).astype(WIDE)
    return lax.psum(low, axis).astype(WIDE)


def gather_rows(part, axis):
    count = lax.axis_size(axis)
    rows = part.shape[0]
    me = lax.axis_index(axis)
    full = jnp.zeros((count * rows,) + part.shape[1:], part.dtype)
    full = lax.dynamic_update_slice_in_dim(full, part, me * rows, 0)
    for step in range(1, count):
        owner = (me - step) % count
        full = lax.dynamic_update_slice_in_dim(full, shifted(part, axis, step), owner * rows, 0)
    return full


def scatter_rows(whole, axis):
    count = lax.axis_size(axis)
    rows = whole.shape[0] // count
    me = lax.axis_index(axis)
    total = lax.dynamic_slice_in_dim(whole, me * rows, rows, 0).astype(WIDE)
    for step in range(1, count):
        piece = lax.dynamic_slice_in_dim(whole, ((me + step) % count) * rows, rows, 0)
        total = total + shifted(piece, axis, step).astype(WIDE)
    return total


def toeplitz_kernel(base_ref, out_ref):
    width = base_ref.shape[2]
    tile = base_ref[0]
    while tile.shape[0] < TILE:
        tile = jnp.concatenate([tile, pltpu.roll(tile, tile.shape[0], 1)], axis=0)
    out_ref[0] = tile.astype(out_ref.dtype)


def toeplitz(base):
    heads, eight, width = base.shape
    return pl.pallas_call(
        toeplitz_kernel,
        grid=(heads,),
        in_specs=[pl.BlockSpec((1, eight, width), lambda h: (h, 0, 0))],
        out_specs=pl.BlockSpec((1, TILE, width), lambda h: (h, 0, 0)),
        out_shape=jax.ShapeDtypeStruct((heads, TILE, width), LOW),
        name="toeplitz",
    )(base)


def head_only(value, head):
    lanes = lax.broadcasted_iota(jnp.int32, value.shape, 1)
    return jnp.where(lanes // DK == head, value, jnp.zeros_like(value))


def bias_starts(first, width):
    return [pl.multiple_of(first - a * TILE + width, TILE) for a in range(width // TILE)]


def score_block(keys, query, tile_ref, head, first):
    scores = right_contract(keys, query)
    if tile_ref is None:
        return scores
    rows = query.shape[0]
    parts = [tile_ref[head, :, pl.ds(s, rows)] for s in bias_starts(first, keys.shape[0])]
    return scores + jnp.concatenate(parts, axis=0).astype(WIDE)


def forward_kernel(biased, rows, base_ref, q_ref, k_ref, v_ref, *rest):
    tile_ref = rest[0] if biased else None
    out_ref, log_ref = rest[-2:]
    total_rows = q_ref.shape[0]
    keys, values = k_ref[...], v_ref[...]
    for block in range(total_rows // rows):
        start = block * rows
        first = base_ref[0] + start
        query = q_ref[start : start + rows, :]
        halves = []
        for head in range(2):
            scores = score_block(keys, head_only(query, head), tile_ref, head, first)
            peak = jnp.max(scores, axis=0, keepdims=True)
            raised = jnp.exp(scores - peak)
            total = jnp.sum(raised, axis=0, keepdims=True)
            result = left_contract(values, raised.astype(LOW)) / total
            halves.append(result[head * DK : head * DK + DK])
            log_ref[0, head : head + 1, start : start + rows] = peak + jnp.log(total)
        out_ref[start : start + rows, :] = jnp.concatenate(halves, axis=0).T.astype(LOW)


def backward_kernel(biased, rows, base_ref, q_ref, k_ref, v_ref, g_ref, log_ref, *rest):
    if biased:
        tile_ref, dq_ref, dk_ref, dv_ref, line_ref, line_sum = rest
    else:
        tile_ref = None
        dq_ref, dk_ref, dv_ref = rest
    total_rows = q_ref.shape[0]
    width = k_ref.shape[0]
    keys, values = k_ref[...], v_ref[...]
    key_grad = [None, None]
    value_grad = [None, None]
    query_halves = [[], []]
    for head in range(2):
        if biased:
            line_sum[...] = jnp.zeros_like(line_sum)
        for block in range(total_rows // rows):
            start = block * rows
            first = base_ref[0] + start
            query = head_only(q_ref[start : start + rows, :], head)
            grad = head_only(g_ref[start : start + rows, :], head)
            scores = score_block(keys, query, tile_ref, head, first)
            probs = jnp.exp(scores - log_ref[0, head : head + 1, start : start + rows])
            prob_grad = right_contract(values, grad)
            product = probs * prob_grad
            score_grad = product - probs * jnp.sum(product, axis=0, keepdims=True)
            low = score_grad.astype(LOW)
            if biased:
                for a, s in enumerate(bias_starts(first, width)):
                    line_sum[:, pl.ds(s, rows)] += score_grad[a * TILE : a * TILE + TILE]
            key_part = matmul(low, query)
            value_part = matmul(probs.astype(LOW), grad)
            key_grad[head] = key_part if block == 0 else key_grad[head] + key_part
            value_grad[head] = value_part if block == 0 else value_grad[head] + value_part
            query_halves[head].append(left_contract(keys, low)[head * DK : head * DK + DK])
        if biased:
            sums = line_sum[...]
            while sums.shape[0] > 8:
                half = sums.shape[0] // 2
                sums = sums[:half] + pltpu.roll(sums[half:], sums.shape[1] - half, 1)
            line_ref[head] = sums
    for block in range(total_rows // rows):
        start = block * rows
        both = jnp.concatenate([query_halves[0][block], query_halves[1][block]], axis=0)
        dq_ref[start : start + rows, :] = both.T.astype(LOW)
    dk_ref[...] = (key_grad[0] + key_grad[1]).astype(LOW)
    dv_ref[...] = (value_grad[0] + value_grad[1]).astype(LOW)


def pair_spec(rows):
    return pl.BlockSpec((rows, PAIR), lambda p: (0, p))


def block_rows(total_rows, width):
    return min(256 if width <= 1024 else 128, total_rows)


def attend(query, keys, values, tiles, base):
    total_rows, columns = query.shape
    width = keys.shape[0]
    rows = block_rows(total_rows, width)
    pairs = columns // PAIR
    biased = tiles is not None
    in_specs = [pl.BlockSpec(memory_space=pltpu.SMEM), pair_spec(total_rows), pair_spec(width), pair_spec(width)]
    operands = [base, query, keys, values]
    if biased:
        in_specs.append(pl.BlockSpec((2,) + tiles.shape[1:], lambda p: (p, 0, 0)))
        operands.append(tiles)
    return pl.pallas_call(
        functools.partial(forward_kernel, biased, rows),
        grid=(pairs,),
        in_specs=in_specs,
        out_specs=[pair_spec(total_rows), pl.BlockSpec((1, 2, total_rows), lambda p: (p, 0, 0))],
        out_shape=[
            jax.ShapeDtypeStruct((total_rows, columns), LOW),
            jax.ShapeDtypeStruct((pairs, 2, total_rows), WIDE),
        ],
        cost_estimate=pl.CostEstimate(
            flops=8 * total_rows * width * columns, bytes_accessed=8 * width * columns,
            transcendentals=total_rows * width * columns // DK,
        ),
        name="attend",
    )(*operands)


def attend_back(query, keys, values, tiles, base, upstream, logs):
    total_rows, columns = query.shape
    width = keys.shape[0]
    rows = block_rows(total_rows, width)
    pairs = columns // PAIR
    biased = tiles is not None
    in_specs = [pl.BlockSpec(memory_space=pltpu.SMEM), pair_spec(total_rows), pair_spec(width), pair_spec(width)]
    in_specs += [pair_spec(total_rows), pl.BlockSpec((1, 2, total_rows), lambda p: (p, 0, 0))]
    operands = [base, query, keys, values, upstream, logs]
    out_specs = [pair_spec(total_rows), pair_spec(width), pair_spec(width)]
    out_shape = [jax.ShapeDtypeStruct((n, columns), LOW) for n in (total_rows, width, width)]
    scratch = []
    if biased:
        span = tiles.shape[2]
        in_specs.append(pl.BlockSpec((2, TILE, span), lambda p: (p, 0, 0)))
        operands.append(tiles)
        out_specs.append(pl.BlockSpec((2, 8, span), lambda p: (p, 0, 0)))
        out_shape.append(jax.ShapeDtypeStruct((2 * pairs, 8, span), WIDE))
        scratch.append(pltpu.VMEM((TILE, span), WIDE))
    return pl.pallas_call(
        functools.partial(backward_kernel, biased, rows),
        grid=(pairs,),
        in_specs=in_specs,
        out_specs=out_specs,
        out_shape=out_shape,
        scratch_shapes=scratch,
        cost_estimate=pl.CostEstimate(
            flops=20 * total_rows * width * columns, bytes_accessed=12 * width * columns,
            transcendentals=total_rows * width * columns // DK,
        ),
        name="attend_back",
    )(*operands)


def body(
    states,
    encoded,
    cotangent,
    bucket_ids,
    norm_gains,
    bias_table,
    self_weights,
    mixer_weight,
    cross_weights,
    blend_weight,
    gate_up,
    down_weight,
):
    shards = lax.axis_size("shard")
    depth = self_weights.shape[1]
    hd = self_weights.shape[2]
    ff = gate_up.shape[2]
    width = bucket_ids.shape[0]
    table_rows, heads = bias_table.shape
    buckets_count = table_rows * shards
    gain_count = norm_gains.shape[0]

    extra = jnp.zeros((depth, TILE), LOW)
    extra = extra.at[:, :gain_count].set(norm_gains.T)
    extra = extra.at[:table_rows, 8 : 8 + heads].set(bias_table)
    first_pack = jnp.concatenate([self_weights[0], self_weights[1], self_weights[2], extra], axis=1)
    second_pack = jnp.concatenate(
        [mixer_weight.T, cross_weights[0], cross_weights[1], cross_weights[2], blend_weight.T], axis=1
    )
    third_pack = jnp.concatenate([gate_up[0], gate_up[1], down_weight.T], axis=1)
    first_full = lax.all_gather(first_pack, "shard", axis=0, tiled=True)
    second_full = lax.all_gather(second_pack, "shard", axis=0, tiled=True)
    third_full = lax.all_gather(third_pack, "shard", axis=0, tiled=True)

    def cut(pack, index, size):
        return pack[:, index * size : index * size + size]

    self_full = [cut(first_full, i, hd) for i in range(3)]
    extra_full = first_full[:, 3 * hd :]
    mixer_t = cut(second_full, 0, hd)
    cross_full = [cut(second_full, i, hd) for i in (1, 2, 3)]
    blend_t = cut(second_full, 4, hd)
    gate_full = [cut(third_full, i, ff) for i in (0, 1)]
    down_t = cut(third_full, 2, ff)

    gains = extra_full[:, :gain_count].astype(WIDE).T
    table = extra_full.reshape(shards, depth, TILE)[:, :table_rows, 8 : 8 + heads].reshape(buckets_count, heads)

    offsets = jnp.arange(width, dtype=jnp.int32)[None, :] - jnp.arange(8, dtype=jnp.int32)[:, None]
    padded = jnp.concatenate([jnp.zeros((8,), jnp.int32), bucket_ids])
    bucket8 = jnp.stack([padded[8 - s : 8 - s + width] for s in range(8)])
    marks = (bucket8[:, :, None] == jnp.arange(buckets_count, dtype=jnp.int32)).astype(WIDE)
    marks = jnp.where((offsets >= 0)[:, :, None], marks, 0.0).reshape(8 * width, buckets_count)
    lines8 = lax.dot_general(
        table, marks.astype(LOW), (((0,), (1,)), ((), ())), preferred_element_type=WIDE
    ).reshape(heads, 8, width)
    lines8 = jnp.where((offsets >= 0)[None], lines8, NEGATIVE)
    line_base = jnp.concatenate([jnp.full((heads, 8, width), NEGATIVE, WIDE), lines8], axis=2)
    tiles = toeplitz(line_base)

    inputs = states[0].astype(WIDE)
    sources = encoded[0]
    upstream_low = cotangent[0]
    upstream = upstream_low.astype(WIDE)
    local_rows = inputs.shape[0]
    base = (lax.axis_index("context") * local_rows).astype(jnp.int32).reshape(1)
    no_base = jnp.zeros((1,), jnp.int32)

    first_norm = normalize(inputs, gains[0]).astype(LOW)
    keys = matmul(first_norm, self_full[1]).astype(LOW)
    values = matmul(first_norm, self_full[2]).astype(LOW)
    query = matmul(first_norm, self_full[0]).astype(LOW)
    all_keys = gather_rows(keys, "context")
    all_values = gather_rows(values, "context")
    attended, head_logs = attend(query, all_keys, all_values, tiles, base)
    after = inputs + pair_sum(right_contract(attended, mixer_t), "tensor")
    source_keys = gather_rows(matmul(sources, cross_full[1]).astype(LOW), "context")
    source_values = gather_rows(matmul(sources, cross_full[2]).astype(LOW), "context")
    second_norm = normalize(after, gains[1]).astype(LOW)
    cross_query = matmul(second_norm, cross_full[0]).astype(LOW)
    cross_attended, cross_logs = attend(cross_query, source_keys, source_values, None, no_base)
    middle = after + pair_sum(right_contract(cross_attended, blend_t), "tensor")
    third_norm = normalize(middle, gains[2]).astype(LOW)
    gate = matmul(third_norm, gate_full[0])
    upper = matmul(third_norm, gate_full[1])
    hidden = geglu(gate, upper).astype(LOW)
    result = middle + pair_sum(right_contract(hidden, down_t), "tensor")

    unused, geglu_pull = jax.vjp(geglu, gate, upper)
    gate_back, upper_back = geglu_pull(matmul(upstream_low, down_t))
    gate_low = gate_back.astype(LOW)
    upper_low = upper_back.astype(LOW)
    third_back = pair_sum(
        right_contract(gate_low, gate_full[0]) + right_contract(upper_low, gate_full[1]), "tensor"
    )
    third_grad = jnp.concatenate(
        [
            left_contract(third_norm, gate_low).astype(LOW),
            left_contract(third_norm, upper_low).astype(LOW),
            left_contract(upstream_low, hidden).astype(LOW),
        ],
        axis=1,
    )
    third_owned = lax.psum_scatter(third_grad, "shard", scatter_dimension=0, tiled=True)
    third_final = pair_sum(third_owned, "context")

    unused, third_pull = jax.vjp(normalize, middle, gains[2])
    middle_part, third_gain = third_pull(third_back)
    middle_grad = upstream + middle_part
    middle_low = middle_grad.astype(LOW)
    cross_out_grad = matmul(middle_low, blend_t).astype(LOW)
    cross_query_grad, key_part, value_part = attend_back(
        cross_query, source_keys, source_values, None, no_base, cross_out_grad, cross_logs
    )
    source_key_low = scatter_rows(key_part, "context").astype(LOW)
    source_value_low = scatter_rows(value_part, "context").astype(LOW)
    second_back = pair_sum(right_contract(cross_query_grad, cross_full[0]), "tensor")
    sources_grad = pair_sum(
        right_contract(source_key_low, cross_full[1]) + right_contract(source_value_low, cross_full[2]),
        "tensor",
    )
    unused, second_pull = jax.vjp(normalize, after, gains[1])
    after_part, second_gain = second_pull(second_back)
    after_grad = middle_grad + after_part
    after_low = after_grad.astype(LOW)
    second_grad = jnp.concatenate(
        [
            left_contract(after_low, attended).astype(LOW),
            left_contract(second_norm, cross_query_grad).astype(LOW),
            left_contract(sources, source_key_low).astype(LOW),
            left_contract(sources, source_value_low).astype(LOW),
            left_contract(middle_low, cross_attended).astype(LOW),
        ],
        axis=1,
    )
    second_owned = lax.psum_scatter(second_grad, "shard", scatter_dimension=0, tiled=True)
    second_final = pair_sum(second_owned, "context")

    attended_grad = matmul(after_low, mixer_t).astype(LOW)
    query_grad, key_sum, value_sum, line_grads = attend_back(
        query, all_keys, all_values, tiles, base, attended_grad, head_logs
    )
    keys_grad = scatter_rows(key_sum, "context").astype(LOW)
    values_grad = scatter_rows(value_sum, "context").astype(LOW)
    table_part = lax.dot_general(
        marks,
        line_grads[:, :, width:].reshape(heads, 8 * width),
        (((0,), (1,)), ((), ())),
        precision=lax.Precision.HIGHEST,
    )
    first_back = pair_sum(
        right_contract(query_grad, self_full[0])
        + right_contract(keys_grad, self_full[1])
        + right_contract(values_grad, self_full[2]),
        "tensor",
    )
    unused, first_pull = jax.vjp(normalize, inputs, gains[0])
    input_part, first_gain = first_pull(first_back)
    inputs_grad = after_grad + input_part
    extra_grad = jnp.zeros((depth * shards, TILE), LOW)
    extra_grad = extra_grad.at[:, :gain_count].set(
        jnp.stack([first_gain, second_gain, third_gain], axis=1).astype(LOW)
    )
    extra_grad = (
        extra_grad.reshape(shards, depth, TILE)
        .at[:, :table_rows, 8 : 8 + heads]
        .set(table_part.astype(LOW).reshape(shards, table_rows, heads))
        .reshape(depth * shards, TILE)
    )
    first_grad = jnp.concatenate(
        [
            left_contract(first_norm, query_grad).astype(LOW),
            left_contract(first_norm, keys_grad).astype(LOW),
            left_contract(first_norm, values_grad).astype(LOW),
            extra_grad,
        ],
        axis=1,
    )
    first_owned = lax.psum_scatter(first_grad, "shard", scatter_dimension=0, tiled=True)
    first_final = pair_sum(first_owned, "context")

    extra_final = first_final[:, 3 * hd :]
    final_gains = extra_final[:, :gain_count].T
    return (
        result.astype(LOW)[None],
        inputs_grad[None],
        sources_grad[None],
        final_gains[:2],
        final_gains[2],
        extra_final[:table_rows, 8 : 8 + heads],
        jnp.stack([cut(first_final, i, hd) for i in range(3)]),
        cut(second_final, 0, hd).T,
        jnp.stack([cut(second_final, i, hd) for i in (1, 2, 3)]),
        cut(second_final, 4, hd).T,
        jnp.stack([cut(third_final, i, ff) for i in (0, 1)]),
        cut(third_final, 2, ff).T,
    )


def solution(mesh):
    in_specs = (
        P("shard", "context", None),
        P("shard", "context", None),
        P("shard", "context", None),
        P(),
        P(None, "shard"),
        P("shard", "tensor"),
        P(None, "shard", "tensor"),
        P("tensor", "shard"),
        P(None, "shard", "tensor"),
        P("tensor", "shard"),
        P(None, "shard", "tensor"),
        P("tensor", "shard"),
    )
    out_specs = (
        P("shard", "context", None),
        P("shard", "context", None),
        P("shard", "context", None),
        P(None, "shard"),
        P("shard"),
        P("shard", "tensor"),
        P(None, "shard", "tensor"),
        P("tensor", "shard"),
        P(None, "shard", "tensor"),
        P("tensor", "shard"),
        P(None, "shard", "tensor"),
        P("tensor", "shard"),
    )
    return jax.shard_map(body, mesh=mesh, in_specs=in_specs, out_specs=out_specs, check_vma=False)
```
